32 devices in a mesh: group: 4 (over y, x), fsdp: 2 (over core), tensor: 4 (over z).
Axes of the slice: x: 2, y: 2, z: 4, core: 2. Of those that a mesh axis runs over, the one named last changes fastest.
Arguments:
- patches: bfloat16 [4, 2, 8, 577, 1024], P('group', None, ('fsdp', 'tensor')), may hold values from -6 to 6
- output_grad: bfloat16 [4, 2, 8, 577, 1024], P('group', None, ('fsdp', 'tensor')), may hold values from -6 to 6
- live_counts: int32 [4, 2, 2], P('group'), may hold values from 1 to 4, as said below
- attn_master: float32 [4, 1024, 1024], P(None, 'fsdp', 'tensor')
- mlp_master: float32 [2, 1024, 4096], P(None, 'fsdp', 'tensor')
- vector_master: float32 [12, 1024], replicated
- attn_moments: float32 [4, 2, 4, 1024, 1024], P('group', None, None, 'fsdp', 'tensor'), as said below
- mlp_moments: float32 [4, 2, 2, 1024, 4096], P('group', None, None, 'fsdp', 'tensor'), as said below
- vector_moments: float32 [4, 2, 12, 1024], P('group'), as said below
- attn_outer: float32 [4, 1024, 1024], P(None, 'fsdp', 'tensor'), may hold values from -0.125 to 0.125
- mlp_outer: float32 [2, 1024, 4096], P(None, 'fsdp', 'tensor'), may hold values from -0.125 to 0.125
- vector_outer: float32 [12, 1024], replicated, may hold values from -0.625 to 0.625
Outputs:
- block_output: bfloat16 [4, 2, 8, 577, 1024], P('group', None, ('fsdp', 'tensor'))
- patches_grad: float32 [4, 2, 8, 577, 1024], P('group', None, ('fsdp', 'tensor'))
- attn_inner: float32 [4, 2, 4, 1024, 1024], P('group', None, None, 'fsdp', 'tensor')
- attn_state: float32 [3, 4, 1024, 1024], P(None, None, 'fsdp', 'tensor')
- attn_copy: bfloat16 [4, 1024, 1024], P(None, 'fsdp', 'tensor')
- mlp_inner: float32 [4, 2, 2, 1024, 4096], P('group', None, None, 'fsdp', 'tensor')
- mlp_state: float32 [3, 2, 1024, 4096], P(None, None, 'fsdp', 'tensor')
- mlp_copy: bfloat16 [2, 1024, 4096], P(None, 'fsdp', 'tensor')
- vector_inner: float32 [4, 2, 12, 1024], P('group')
- vector_state: float32 [3, 12, 1024], replicated
- vector_copy: bfloat16 [12, 1024], replicated
The draws below stay inside these ranges and needn't reach their ends.
Inputs may be any that keep to these rules, and one draw needn't show every extreme that they name: live_counts[g, m, f] images are live, and they stand first, among the f-th block of 4 image slots of micro-batch m in group g; some entry equals 4. `attn_moments`: second moments are positive. `mlp_moments`: second moments are positive. `vector_moments`: second moments are positive.
All inputs are finite; a program needn't handle non-finite values.
Results may differ from the reference program's by a relative error of at most 0.012.
The reference program's roundings to bfloat16 on the way count: a program that leaves them out, or rounds other values in their place, can miss the bound.
Values may be sent and summed in bfloat16 or wider, within the bound.
A program may use at most 320 MiB of HBM per device.

```python
import math
import jax
import jax.numpy as jnp
from jax import lax

D = 1024
HD = 64
FF = 4096
SEQ = 577
MICRO = 2
STEP = 8
IMG_DEV = 4
IMAGES = 8
GROUPS = 4
NV = 12


def draw_live_counts(key, part):
    owners = IMAGES // IMG_DEV
    drawn = jax.random.randint(key, (GROUPS, MICRO, owners), 1, IMG_DEV + 1)
    picked = jax.random.randint(jax.random.fold_in(key, 11), (3,), 0, 1 << 20)
    return drawn.at[picked[0] % GROUPS, picked[1] % MICRO, picked[2] % owners].set(IMG_DEV).astype(jnp.int32)


def draw_attn_master(key, part):
    factor = jnp.array([1.3, 1.3, 1.0, 8.0], jnp.float32) * D ** (-0.5)
    noise = jax.random.truncated_normal(key, -4.0, 4.0, (4, D, D), jnp.float32)
    return noise * factor[:, None, None]


def draw_mlp_master(key, part):
    factor = jnp.array([D ** (-0.5), FF ** (-0.5)], jnp.float32)
    noise = jax.random.truncated_normal(key, -4.0, 4.0, (2, D, FF), jnp.float32)
    return noise * factor[:, None, None]


def draw_vector_master(key, part):
    gain_rows = jax.random.uniform(key, (NV, D), jnp.float32, 0.5, 1.5)
    shifts = jax.random.truncated_normal(jax.random.fold_in(key, 1), -4.0, 4.0, (NV, D), jnp.float32)
    row_index = jnp.arange(NV)[:, None]
    spread = jnp.where(row_index == 5, 0.1, 0.3)
    is_gain = (row_index == 0) | (row_index == 2)
    return jnp.where(is_gain, gain_rows, shifts * spread)


def moments_from(key, factor, shape):
    magnitude = factor * math.sqrt(MICRO * IMAGES * SEQ * 0.6)
    first_moment = jax.random.normal(jax.random.fold_in(key, 1), shape, jnp.float32) * magnitude * (0.1 / 0.9)
    spread = jnp.exp(jax.random.uniform(jax.random.fold_in(key, 2), shape, jnp.float32, 0.0, math.log(4.0)))
    second_moment = magnitude * magnitude * (0.05 / 0.95) * spread
    return jnp.stack([first_moment, second_moment], axis=1)


def draw_attn_moments(key, part):
    factor = jnp.array([1.2, 1.2, 0.8, 0.2], jnp.float32)[None, :, None, None]
    return moments_from(key, factor, (GROUPS, 4, D, D))


def draw_mlp_moments(key, part):
    factor = jnp.array([0.35, 0.6], jnp.float32)[None, :, None, None]
    return moments_from(key, factor, (GROUPS, 2, D, FF))


def draw_vector_moments(key, part):
    leading = jnp.array([2.3, 2.3, 0.7, 0.7, 1.2, 0.8, 1.5, 1.0], jnp.float32)
    factor = jnp.concatenate([leading, jnp.full((NV - 8,), 0.35, jnp.float32)])[None, :, None]
    return moments_from(key, factor, (GROUPS, NV, D))


def level_of(own_key, dims, split, low, largest):
    gain, own = 1.0, jax.random.fold_in(own_key, 6)
    for axis_at, shards_of in split:
        heights = jnp.exp(jax.random.uniform(jax.random.fold_in(own, axis_at), (shards_of,), jnp.float32, low / len(split), largest / len(split)))
        gain = gain * jnp.repeat(heights, dims[axis_at] // shards_of).reshape([-1 if axis == axis_at else 1 for axis in range(len(dims))])
    return gain


def gaussian(own_key, extent, scale, bound, cuts=(), dtype=jnp.bfloat16):
    values = scale * jax.random.normal(own_key, extent, jnp.float32)
    if cuts:
        values = values * level_of(own_key, extent, cuts, -0.22, 0.18)
    return jnp.clip(values, -bound, bound).astype(dtype)


def setup_inputs(seed: int = 0) -> dict:
    streams_of = jax.random.split(jax.random.key(seed), 13)
    return {
        "patches": gaussian(streams_of[0], (GROUPS, MICRO, IMAGES, SEQ, D), 1.0, 6.0, ((0, 4), (2, 8))),
        "output_grad": gaussian(streams_of[1], (GROUPS, MICRO, IMAGES, SEQ, D), 1.0, 6.0, ((0, 4), (2, 8))),
        "live_counts": draw_live_counts(jax.random.fold_in(streams_of[12], 71), 0),
        "attn_master": draw_attn_master(jax.random.fold_in(streams_of[12], 71), 0),
        "mlp_master": draw_mlp_master(jax.random.fold_in(streams_of[12], 71), 0),
        "vector_master": draw_vector_master(jax.random.fold_in(streams_of[12], 71), 0),
        "attn_moments": draw_attn_moments(jax.random.fold_in(streams_of[12], 71), 0),
        "mlp_moments": draw_mlp_moments(jax.random.fold_in(streams_of[12], 71), 0),
        "vector_moments": draw_vector_moments(jax.random.fold_in(streams_of[12], 71), 0),
        "attn_outer": gaussian(streams_of[9], (4, D, D), 0.02, 0.125, ((1, 2), (2, 4)), jnp.float32),
        "mlp_outer": gaussian(streams_of[10], (2, D, FF), 0.02, 0.125, ((1, 2), (2, 4)), jnp.float32),
        "vector_outer": gaussian(streams_of[11], (NV, D), 0.1, 0.625, (), jnp.float32),
    }


EPSILON = 1e-06
PRECISE = lax.Precision.HIGHEST
INNER_RATE = 0.02
VECTOR_RATE = 0.2
WEIGHT_DECAY = 0.1
OUTER_RATE = 0.7
OUTER_MOMENTUM = 0.9

@jax.custom_vjp
def low(v):
    return lax.optimization_barrier(v.astype(jnp.bfloat16)).astype(jnp.float32)

@jax.custom_vjp
def low_back(v):
    return v

def low_keep(v):
    return (low(v), None)

def low_pass(kept, grad):
    return (grad,)

def back_keep(v):
    return (v, None)

def back_low(kept, grad):
    return (low(grad),)
low.defvjp(low_keep, low_pass)
low_back.defvjp(back_keep, back_low)

def normalize(source, gain_row, shift_row):
    centre = source - lax.optimization_barrier(jnp.mean(source, axis=-1, keepdims=True))
    spread = lax.optimization_barrier(jnp.mean(centre * centre, axis=-1, keepdims=True))
    return centre * lax.rsqrt(spread + EPSILON) * gain_row + shift_row

def inner_adamw(master, gradient, moments, step_rate, decay_rate):
    first_moment = 0.9 * moments[0] + 0.1 * gradient
    second_moment = 0.95 * moments[1] + 0.05 * gradient * gradient
    step_ratio = first_moment / (1.0 - 0.9 ** STEP) / (jnp.sqrt(second_moment / (1.0 - 0.95 ** STEP)) + 1e-08)
    return (master - step_rate * (step_ratio + decay_rate * master), second_moment)

def outer_nesterov(master, outer_old, difference):
    momentum = OUTER_MOMENTUM * outer_old + difference
    updated = master - OUTER_RATE * (difference + OUTER_MOMENTUM * momentum)
    return (jnp.stack([difference, momentum, updated]), updated.astype(jnp.bfloat16))

def block_forward(attn, mlp_weights, vector, row_block):
    image_count, seq_len, width = row_block.shape
    head_count = width // HD
    score_scale = HD ** (-0.5)
    normed_one = low(normalize(row_block, vector[0], vector[1]))
    queries = low(low_back(jnp.einsum('isd,de->ise', normed_one, attn[0], precision=PRECISE) + vector[4]))
    keys_low = low(low_back(jnp.einsum('isd,de->ise', normed_one, attn[1], precision=PRECISE)))
    values_low = low(low_back(jnp.einsum('isd,de->ise', normed_one, attn[2], precision=PRECISE) + vector[5]))
    shape_heads = (image_count, seq_len, head_count, HD)
    scores = low_back(jnp.einsum('iqhe,ikhe->ihqk', queries.reshape(shape_heads), keys_low.reshape(shape_heads), precision=PRECISE) * score_scale)
    probs_full = jax.nn.softmax(scores, axis=-1)
    attended = jnp.einsum('ihqk,ikhe->iqhe', low(probs_full), values_low.reshape(shape_heads), precision=PRECISE)
    attended = low(low_back(attended.reshape(image_count, seq_len, width)))
    branch_one = low_back(jnp.einsum('ise,de->isd', attended, attn[3], precision=PRECISE))
    resid_one = row_block + branch_one + vector[6]
    normed_two = low(normalize(resid_one, vector[2], vector[3]))
    pre_act = low_back(jnp.einsum('isd,df->isf', normed_two, mlp_weights[0], precision=PRECISE) + vector[8:].reshape(-1))
    hidden = low(jax.nn.gelu(pre_act, approximate=False))
    branch_two = low_back(jnp.einsum('isf,df->isd', hidden, mlp_weights[1], precision=PRECISE))
    return resid_one + branch_two + vector[7]

def reference(patches, output_grad, live_counts, attn_master, mlp_master, vector_master, attn_moments, mlp_moments, vector_moments, attn_outer, mlp_outer, vector_outer):
    attn_low = low(attn_master)
    mlp_low = low(mlp_master)
    slot_index = jnp.arange(IMAGES)
    block_size = math.gcd(MICRO * IMAGES, 4)
    mixed_groups = []
    input_groups = []
    attn_inner = []
    mlp_inner = []
    vector_inner = []
    attn_diff = jnp.zeros_like(attn_master)
    mlp_diff = jnp.zeros_like(mlp_master)
    vector_diff = jnp.zeros_like(vector_master)
    for group_index in range(GROUPS):
        alive = (slot_index[None, :] % IMG_DEV < live_counts[group_index][:, slot_index // IMG_DEV]).astype(jnp.float32)
        row_blocks = patches[group_index].astype(jnp.float32).reshape(-1, block_size, SEQ, D)
        cotangents = output_grad[group_index].astype(jnp.float32).reshape(-1, block_size, SEQ, D)
        alive_blocks = alive.reshape(-1, block_size)

        def scan_step(totals_now, block_item):
            rows_now, back_now, alive_block = block_item

            def forward(attn, mlp_weights, vector, inputs):
                return block_forward(attn, mlp_weights, vector, inputs) * alive_block[:, None, None]
            result, pullback = jax.vjp(forward, attn_low, mlp_low, vector_master, rows_now)
            gradients = pullback(back_now)
            totals_next = (totals_now[0] + gradients[0], totals_now[1] + gradients[1], totals_now[2] + gradients[2])
            return (totals_next, (result.astype(jnp.bfloat16), gradients[3]))
        zero_sums = (jnp.zeros_like(attn_master), jnp.zeros_like(mlp_master), jnp.zeros_like(vector_master))
        grad_sums, block_outputs = lax.scan(scan_step, zero_sums, (row_blocks, cotangents, alive_blocks))
        mixed_groups.append(block_outputs[0].reshape(MICRO, IMAGES, SEQ, D))
        input_groups.append(block_outputs[1].reshape(MICRO, IMAGES, SEQ, D))
        new_attn, second_attn = inner_adamw(attn_master, grad_sums[0], attn_moments[group_index], INNER_RATE, WEIGHT_DECAY)
        new_mlp, second_mlp = inner_adamw(mlp_master, grad_sums[1], mlp_moments[group_index], INNER_RATE, WEIGHT_DECAY)
        new_vector, second_vector = inner_adamw(vector_master, grad_sums[2], vector_moments[group_index], VECTOR_RATE, 0.0)
        attn_inner.append(jnp.stack([grad_sums[0], second_attn]))
        mlp_inner.append(jnp.stack([grad_sums[1], second_mlp]))
        vector_inner.append(jnp.stack([grad_sums[2], second_vector]))
        attn_diff = attn_diff + (attn_master - new_attn)
        mlp_diff = mlp_diff + (mlp_master - new_mlp)
        vector_diff = vector_diff + (vector_master - new_vector)
    attn_state, attn_copy = outer_nesterov(attn_master, attn_outer, attn_diff / GROUPS)
    mlp_state, mlp_copy = outer_nesterov(mlp_master, mlp_outer, mlp_diff / GROUPS)
    vector_state, vector_copy = outer_nesterov(vector_master, vector_outer, vector_diff / GROUPS)
    return (jnp.stack(mixed_groups), jnp.stack(input_groups), jnp.stack(attn_inner), attn_state, attn_copy, jnp.stack(mlp_inner), mlp_state, mlp_copy, jnp.stack(vector_inner), vector_state, vector_copy)
```

```python
from functools import partial

import jax
import jax.numpy as jnp
from jax import lax
from jax.sharding import PartitionSpec as P

HD = 64
FF = 4096
STEP = 8


EPSILON = 1e-06
INNER_RATE = 0.02
VECTOR_RATE = 0.2
WEIGHT_DECAY = 0.1
OUTER_RATE = 0.7
OUTER_MOMENTUM = 0.9


def normalize(source, gain_row, shift_row):
    centre = source - jnp.mean(source, axis=-1, keepdims=True)
    spread = jnp.mean(centre * centre, axis=-1, keepdims=True)
    return centre * lax.rsqrt(spread + EPSILON) * gain_row + shift_row


def gelu_exact(source):
    return jax.nn.gelu(source, approximate=False)


def gelu_slope(source):
    return (
        0.5 * (1.0 + lax.erf(source * 0.7071067811865476))
        + source * jnp.exp(-0.5 * source * source) * 0.3989422804014327
    )


def inner_adamw(master, gradient, moments, step_rate, decay_rate):
    first_moment = 0.9 * moments[0] + 0.1 * gradient
    second_moment = 0.95 * moments[1] + 0.05 * gradient * gradient
    step_ratio = (
        first_moment / (1.0 - 0.9**STEP) / (jnp.sqrt(second_moment / (1.0 - 0.95**STEP)) + 1e-08)
    )
    return (master - step_rate * (step_ratio + decay_rate * master), second_moment)


def outer_nesterov(master, outer_old, difference):
    momentum = OUTER_MOMENTUM * outer_old + difference
    updated = master - OUTER_RATE * (difference + OUTER_MOMENTUM * momentum)
    return (jnp.stack([difference, momentum, updated]), updated.astype(jnp.bfloat16))


def attend_forward(score_scale, operands):
    queries_low, keys_low, values_low = operands
    scores = (
        jnp.einsum("qhe,khe->hqk", queries_low, keys_low, preferred_element_type=jnp.float32)
        * score_scale
    )
    highest = jnp.max(scores, axis=-1, keepdims=True)
    exponent = jnp.exp(scores - highest)
    totals = jnp.sum(exponent, axis=-1, keepdims=True)
    probs_low = (exponent / totals).astype(jnp.bfloat16)
    attended = jnp.einsum("hqk,khe->qhe", probs_low, values_low, preferred_element_type=jnp.float32)
    return (attended.astype(jnp.bfloat16), (highest + jnp.log(totals))[..., 0])


def attend_backward(score_scale, operands):
    queries_low, keys_low, values_low, log_totals, grad_attended = operands
    scores = (
        jnp.einsum("qhe,khe->hqk", queries_low, keys_low, preferred_element_type=jnp.float32)
        * score_scale
    )
    probs_full = jnp.exp(scores - log_totals[..., None])
    grad_probs = jnp.einsum(
        "qhe,khe->hqk", grad_attended, values_low, preferred_element_type=jnp.float32
    )
    grad_values = jnp.einsum(
        "hqk,qhe->khe",
        probs_full.astype(jnp.bfloat16),
        grad_attended,
        preferred_element_type=jnp.float32,
    )
    weighted = jnp.sum(probs_full * grad_probs, axis=-1, keepdims=True)
    grad_scores = (probs_full * (grad_probs - weighted)).astype(jnp.bfloat16)
    grad_queries = (
        jnp.einsum("hqk,khe->qhe", grad_scores, keys_low, preferred_element_type=jnp.float32)
        * score_scale
    )
    grad_keys = (
        jnp.einsum("hqk,qhe->khe", grad_scores, queries_low, preferred_element_type=jnp.float32)
        * score_scale
    )
    return (
        grad_queries.astype(jnp.bfloat16),
        grad_keys.astype(jnp.bfloat16),
        grad_values.astype(jnp.bfloat16),
    )


def local(
    patches,
    output_grad,
    live_counts,
    attn_master,
    mlp_master,
    vector_master,
    attn_moments,
    mlp_moments,
    vector_moments,
    attn_outer,
    mlp_outer,
    vector_outer,
):
    narrow = jnp.bfloat16
    single = jnp.float32
    tensor_index = lax.axis_index("tensor")
    fsdp_index = lax.axis_index("fsdp")
    micro_count = patches.shape[1]
    local_images = patches.shape[2]
    seq_len = patches.shape[3]
    width = patches.shape[4]
    score_scale = HD ** (-0.5)
    tensor_size = lax.axis_size("tensor")

    def whole(master):
        shards = lax.all_gather(master.astype(narrow), ("fsdp", "tensor"), axis=0, tiled=False)
        f_size = lax.axis_size("fsdp")
        shards = shards.reshape((f_size, tensor_size) + master.shape)
        shards = jnp.transpose(shards, (2, 0, 3, 1, 4))
        return shards.reshape(master.shape[0], f_size * master.shape[1], tensor_size * master.shape[2])

    attn_all = whole(attn_master)
    mlp_all = whole(mlp_master)
    owner_counts = jnp.sum(
        jnp.where(jnp.arange(live_counts.shape[2]) == fsdp_index, live_counts[0], 0), axis=-1
    )
    slot_index = tensor_index * local_images + jnp.arange(local_images)
    alive = (slot_index[None, :] < owner_counts[:, None]).astype(single).reshape(-1)[:, None, None]
    image_count = micro_count * local_images
    heads = width // HD
    shape_heads = (image_count, seq_len, heads, HD)
    inputs = patches.reshape(image_count, seq_len, width).astype(single)
    grad_out = alive * output_grad.reshape(image_count, seq_len, width).astype(single)
    grad_two = grad_out.astype(narrow)
    normed_one = normalize(inputs, vector_master[0], vector_master[1]).astype(narrow)

    def dot_in(rows, weight):
        return jnp.einsum("isd,de->ise", rows, weight, preferred_element_type=single)

    def dot_out(rows, weight):
        return jnp.einsum("ise,de->isd", rows, weight, preferred_element_type=single)

    def outer(rows, cols):
        return jnp.einsum("isd,ise->de", rows, cols, preferred_element_type=single).astype(narrow)

    queries_low = (dot_in(normed_one, attn_all[0]) + vector_master[4]).astype(narrow)
    keys_low = dot_in(normed_one, attn_all[1]).astype(narrow)
    values_low = (dot_in(normed_one, attn_all[2]) + vector_master[5]).astype(narrow)
    queries_low = queries_low.reshape(shape_heads)
    keys_low = keys_low.reshape(shape_heads)
    values_low = values_low.reshape(shape_heads)
    attended, log_totals = lax.map(
        partial(attend_forward, score_scale), (queries_low, keys_low, values_low)
    )
    attended = attended.reshape(image_count, seq_len, width)
    resid_one = inputs + dot_out(attended, attn_all[3]) + vector_master[6]
    normed_two = normalize(resid_one, vector_master[2], vector_master[3]).astype(narrow)
    pre_act = dot_in(normed_two, mlp_all[0]) + vector_master[8:].reshape(-1)
    hidden = gelu_exact(pre_act).astype(narrow)
    branch_two = dot_out(hidden, mlp_all[1])
    mixed = (alive * (resid_one + branch_two + vector_master[7])).astype(narrow)
    fc_out = outer(grad_two, hidden)
    grad_pre = (dot_in(grad_two, mlp_all[1]) * gelu_slope(pre_act)).astype(narrow)
    fc_in = outer(normed_two, grad_pre)
    grad_normed_two = dot_out(grad_pre, mlp_all[0])
    unused_two, norm_pull_two = jax.vjp(normalize, resid_one, vector_master[2], vector_master[3])
    back_resid, gain_two, shift_two = norm_pull_two(grad_normed_two)
    grad_resid = grad_out + back_resid
    grad_one = grad_resid.astype(narrow)
    out_grad = outer(grad_one, attended)
    grad_attended = dot_in(grad_one, attn_all[3]).astype(narrow).reshape(shape_heads)
    grad_queries, grad_keys, grad_values = lax.map(
        partial(attend_backward, score_scale),
        (queries_low, keys_low, values_low, log_totals, grad_attended),
    )
    grad_queries = grad_queries.reshape(image_count, seq_len, width)
    grad_keys = grad_keys.reshape(image_count, seq_len, width)
    grad_values = grad_values.reshape(image_count, seq_len, width)
    grad_normed_one = (
        dot_out(grad_queries, attn_all[0])
        + dot_out(grad_keys, attn_all[1])
        + dot_out(grad_values, attn_all[2])
    )
    unused_one, norm_pull_one = jax.vjp(normalize, inputs, vector_master[0], vector_master[1])
    back_inputs, gain_one, shift_one = norm_pull_one(grad_normed_one)
    input_grad = grad_resid + back_inputs

    def owned(whole_grad, shape):
        f_size = lax.axis_size("fsdp")
        parts = whole_grad.reshape(shape[0], f_size, shape[1], tensor_size, shape[2])
        parts = jnp.transpose(parts, (1, 3, 0, 2, 4))
        mine = lax.psum_scatter(parts, "fsdp", scatter_dimension=0, tiled=False)
        return lax.psum_scatter(mine, "tensor", scatter_dimension=0, tiled=False).astype(single)

    mlp_grad = owned(jnp.stack([fc_in, fc_out]), mlp_master.shape)
    attn_grad = owned(
        jnp.stack(
            [
                outer(normed_one, grad_queries),
                outer(normed_one, grad_keys),
                outer(normed_one, grad_values),
                out_grad,
            ]
        ),
        attn_master.shape,
    )

    def total(rows):
        return jnp.sum(rows.astype(single), axis=(0, 1))

    vector_part = jnp.concatenate(
        [
            jnp.stack(
                [
                    gain_one,
                    shift_one,
                    gain_two,
                    shift_two,
                    total(grad_queries),
                    total(grad_values),
                    total(grad_resid),
                    total(grad_out),
                ]
            ),
            total(grad_pre).reshape(-1, width),
        ],
        0,
    )
    vector_grad = lax.psum(vector_part, ("fsdp", "tensor"))
    new_attn, second_attn = inner_adamw(
        attn_master, attn_grad, attn_moments[0], INNER_RATE, WEIGHT_DECAY
    )
    new_mlp, second_mlp = inner_adamw(
        mlp_master, mlp_grad, mlp_moments[0], INNER_RATE, WEIGHT_DECAY
    )
    new_vector, second_vector = inner_adamw(
        vector_master, vector_grad, vector_moments[0], VECTOR_RATE, 0.0
    )
    groups = lax.axis_size("group")

    def group_sum(difference):
        flat = difference.astype(narrow).reshape((groups, -1, difference.shape[-1]))
        mine = lax.psum_scatter(flat, "group", scatter_dimension=0, tiled=False)
        summed = lax.all_gather(mine, "group", axis=0, tiled=False)
        return summed.reshape(difference.shape).astype(single)

    diff_attn = group_sum(attn_master - new_attn)
    diff_mlp = group_sum(mlp_master - new_mlp)
    diff_vector = lax.psum(vector_master - new_vector, "group")
    attn_state, attn_copy = outer_nesterov(attn_master, attn_outer, diff_attn / groups)
    mlp_state, mlp_copy = outer_nesterov(mlp_master, mlp_outer, diff_mlp / groups)
    vector_state, vector_copy = outer_nesterov(vector_master, vector_outer, diff_vector / groups)
    block_output = mixed.reshape(patches.shape)
    patches_grad = input_grad.reshape(patches.shape)
    attn_inner = jnp.stack([attn_grad, second_attn])[None]
    mlp_inner = jnp.stack([mlp_grad, second_mlp])[None]
    vector_inner = jnp.stack([vector_grad, second_vector])[None]
    return (
        block_output,
        patches_grad,
        attn_inner,
        attn_state,
        attn_copy,
        mlp_inner,
        mlp_state,
        mlp_copy,
        vector_inner,
        vector_state,
        vector_copy,
    )


def solution(mesh):
    placed = (
        P("group", None, ("fsdp", "tensor"), None, None),
        P("group", None, ("fsdp", "tensor"), None, None),
        P("group", None, None),
        P(None, "fsdp", "tensor"),
        P(None, "fsdp", "tensor"),
        P(),
        P("group", None, None, "fsdp", "tensor"),
        P("group", None, None, "fsdp", "tensor"),
        P("group", None, None, None),
        P(None, "fsdp", "tensor"),
        P(None, "fsdp", "tensor"),
        P(),
    )
    return jax.shard_map(
        local,
        mesh=mesh,
        in_specs=placed,
        out_specs=(
            P("group", None, ("fsdp", "tensor"), None, None),
            P("group", None, ("fsdp", "tensor"), None, None),
            P("group", None, None, "fsdp", "tensor"),
            P(None, None, "fsdp", "tensor"),
            P(None, "fsdp", "tensor"),
            P("group", None, None, "fsdp", "tensor"),
            P(None, None, "fsdp", "tensor"),
            P(None, "fsdp", "tensor"),
            P("group", None, None, None),
            P(),
            P(),
        ),
        check_vma=False,
    )
```
